256 devices in a mesh: rep: 2 (over core), dp: 128 (over x, y, z).
Axes of the slice: x: 4, y: 4, z: 8, core: 2. Of those that a mesh axis runs over, the one named last changes fastest.
Arguments:
- a: bfloat16 [256, 2, 4096, 768], P(('rep', 'dp')), parts along dimension 0
- g: bfloat16 [256, 2, 4096, 1792], P(('rep', 'dp')), parts along dimension 0
Outputs:
- output: bfloat16 [4, 768, 1792], P('rep'), parts along dimension 0
There are 2 independent parts. The reference program is written for one: setup_inputs(seed, part) draws one part's arguments, and reference() takes and returns one part's arrays. A program takes and returns all parts, laid end to end along the dimension named above; each array names one.
All inputs are finite; a program needn't handle non-finite values.
Results may differ from the reference program's by a relative error of at most 0.012.
Values are sent between devices in bfloat16 or wider.
A program may use at most 768 MiB of HBM per device.

```python
import jax
import jax.numpy as jnp
from jax import lax

DEVICES = 128
MATRICES = 2
TOKENS = 4096
D = 768
FF = 1792


def setup_inputs(seed: int = 0, part: int = 0) -> dict:
    ka, kg, ks = (jax.random.fold_in(k, part) for k in jax.random.split(jax.random.key(seed), 3))
    size = 2.0 ** jax.random.uniform(ks, (DEVICES, MATRICES, 1, 1), jnp.float32, -1.0, 1.0)
    a = jax.random.normal(ka, (DEVICES, MATRICES, TOKENS, D), jnp.float32)
    g = size * jax.random.normal(kg, (DEVICES, MATRICES, TOKENS, FF), jnp.float32) * (DEVICES * TOKENS) ** -0.5
    return {"a": a.astype(jnp.bfloat16), "g": g.astype(jnp.bfloat16)}


def reference(a, g):
    def take(so_far, one):
        term = jnp.einsum("ntd,ntf->ndf", *one, preferred_element_type=jnp.float32).astype(jnp.bfloat16)
        return so_far + term.astype(jnp.float32), None

    return lax.scan(take, jnp.zeros((MATRICES, D, FF), jnp.float32), (a, g))[0].astype(jnp.bfloat16)
```

```python
import jax
import jax.numpy as jnp
from jax import lax
from jax.sharding import PartitionSpec as P


def solution(mesh):
    def body(a, g):
        outs = []
        for n in range(2):
            t = lax.dot_general(a[0, n], g[0, n], (((0,), (0,)), ((), ())), preferred_element_type=jnp.float32).astype(jnp.bfloat16)
            outs.append(lax.psum(t, "dp"))
        return jnp.stack(outs)

    return jax.shard_map(body, mesh=mesh, in_specs=(P(("rep", "dp")),) * 2, out_specs=P("rep"), check_vma=False)
```

```python
import jax
import jax.numpy as jnp
from jax import lax
from jax.experimental import pallas as pl
from jax.experimental.pallas import tpu as pltpu
from jax.sharding import PartitionSpec as P

X, Y, Z = 4, 4, 8
U, L = 48, 128
UNITS = 32
W = 2 * L
AFTER = (0, 3, 5, 7, 9, 12, 15, 17, 21, 26)
ORDER = (3, 2, 8, 1, 6, 5, 4, 9, 7)
GBUF = 4
MB = 384
bf16, f32 = jnp.bfloat16, jnp.float32


def kernel(a_hbm, g_hbm, outb, abuf, gbuf, term, recv1, acc, part, recv2, exch,
           asem, gsem, ssem, r1sem, r2sem, xsem, g2sem, g1sem):
    mats, tokens, d = a_hbm.shape
    per = g_hbm.shape[2] // W
    pieces = mats * per
    me = lax.axis_index("dp")
    x, y, z = me // (Y * Z), (me // Z) % Y, me % Z

    def load_a(n):
        return pltpu.make_async_copy(a_hbm.at[n], abuf.at[n], asem.at[n])

    def load_g(t):
        col = pl.multiple_of((t % per) * W, W)
        slot = t % GBUF
        return pltpu.make_async_copy(g_hbm.at[t // per, :, pl.ds(col, W)], gbuf.at[slot], gsem.at[slot])

    def compute(t):
        n, slot = t // per, t % GBUF
        load_g(t).wait()

        @pl.when(t % per == 0)
        def _():
            load_a(n).wait()

        for m in range(0, d, MB):
            s = lax.dot_general(abuf[n, :, m : m + MB], gbuf[slot], (((0,), (0,)), ((), ())), preferred_element_type=f32).astype(bf16)
            for h in range(2):
                u = h * (UNITS // 2) + m // U
                term[t, u : u + MB // U] = s[:, h * L : (h + 1) * L].reshape(MB // U, U, L)

    def place(p):
        odd = p % 2
        s = 1 - 2 * ((p // 2) % 2)
        c1, st1 = x + odd * (y - x), Y * Z - odd * (Y * Z - Z)
        c3, st3 = y + odd * (x - y), Z + odd * (Y * Z - Z)

        def on1(k):
            return (c1 + k + 8) % 4

        def on3(k):
            return (c3 + k + 8) % 4

        def onz(k):
            return (z + k + 8) % 8

        dev1 = lambda k: me + (on1(k) - c1) * st1
        dev3 = lambda k: me + (on3(k) - c3) * st3
        devz = lambda k: me + onz(k) - z
        return s, c1, c3, on1, on3, onz, dev1, dev3, devz

    def send(src, dst, p, sem, dev):
        pltpu.make_async_remote_copy(
            src_ref=src, dst_ref=dst, send_sem=ssem.at[p], recv_sem=sem,
            device_id={"dp": dev}, device_id_type=pl.DeviceIdType.MESH,
        ).start()

    def wait(ref, sem):
        pltpu.make_async_copy(ref, ref, sem).wait()

    def chunk(c):
        return pl.ds(c * Z, Z)

    def half(c, h):
        return pl.ds(c * Z + h * (Z // 2), Z // 2)

    def step0(p):
        s, c1, c3, on1, on3, onz, dev1, dev3, devz = place(p)
        for h, o in ((0, 1), (1, -1)):
            send(term.at[p, half(on1(2), h)], recv1.at[p, h], p, r1sem.at[p, h], dev1(-o))
        for h, o in ((0, 1), (1, -1)):
            send(term.at[p, half(on1(o), h)], recv1.at[p, 2 + h], p, r1sem.at[p, 2 + h], dev1(o))

    def step1(p):
        s, c1, c3, on1, on3, onz, dev1, dev3, devz = place(p)
        for h, o in ((0, 1), (1, -1)):
            wait(recv1.at[p, h], r1sem.at[p, h])
            base = on1(-o) * Z + h * (Z // 2)
            for u in range(Z // 2):
                term[p, base + u] = (term[p, base + u].astype(f32) + recv1[p, h, u].astype(f32)).astype(bf16)
            send(term.at[p, half(on1(-o), h)], recv1.at[p, 4 + h], p, r1sem.at[p, 4 + h], dev1(-o))

    def step2(p):
        s, c1, c3, on1, on3, onz, dev1, dev3, devz = place(p)
        for k in range(2, 6):
            wait(recv1.at[p, k], r1sem.at[p, k])
        for u in range(Z):
            h, w = divmod(u, Z // 2)
            v = term[p, c1 * Z + u].astype(f32) + recv1[p, 2 + h, w].astype(f32) + recv1[p, 4 + h, w].astype(f32)
            acc[p, u] = v
            part[p, u] = v.astype(bf16)
        send(part.at[p, onz(4)], recv2.at[p, 0], p, r2sem.at[p, 0], devz(-2 * s))
        send(part.at[p, onz(-3 * s)], recv2.at[p, 1], p, r2sem.at[p, 1], devz(-s))
        send(part.at[p, onz(3 * s)], recv2.at[p, 2], p, r2sem.at[p, 2], devz(s))
        send(part.at[p, onz(-s)], recv2.at[p, 3], p, r2sem.at[p, 3], devz(-s))
        send(part.at[p, onz(s)], recv2.at[p, 4], p, r2sem.at[p, 4], devz(s))

    def step3(p):
        s, c1, c3, on1, on3, onz, dev1, dev3, devz = place(p)
        for k in range(3):
            wait(recv2.at[p, k], r2sem.at[p, k])
        far, near = onz(-2 * s), onz(2 * s)
        part[p, far] = (acc[p, far] + recv2[p, 0].astype(f32) + recv2[p, 1].astype(f32)).astype(bf16)
        part[p, near] = (acc[p, near] + recv2[p, 2].astype(f32)).astype(bf16)
        send(part.at[p, far], recv2.at[p, 5], p, r2sem.at[p, 5], devz(-2 * s))
        send(part.at[p, near], recv2.at[p, 6], p, r2sem.at[p, 6], devz(2 * s))

    def step4(p):
        s, c1, c3, on1, on3, onz, dev1, dev3, devz = place(p)
        for k in range(3, 7):
            wait(recv2.at[p, k], r2sem.at[p, k])
        v = acc[p, z]
        for k in range(3, 7):
            v = v + recv2[p, k].astype(f32)
        exch[p, c3] = v.astype(bf16)
        for k in range(1, 4):
            send(exch.at[p, c3], exch.at[p, c3], p, xsem.at[p, k - 1], dev3(k))

    def step5(p):
        s, c1, c3, on1, on3, onz, dev1, dev3, devz = place(p)
        for k in range(1, 4):
            wait(exch.at[p, on3(-k)], xsem.at[p, k - 1])
        v = exch[p, 0].astype(f32)
        for k in range(1, 4):
            v = v + exch[p, k].astype(f32)
        u = c1 * Z + z
        outb[p, u] = v.astype(bf16)
        for k, h in enumerate((-2, 2, -1, 1)):
            send(outb.at[p, u], outb.at[p, u], p, g2sem.at[p, k], devz(h * s))

    def step6(p):
        s, c1, c3, on1, on3, onz, dev1, dev3, devz = place(p)
        far, near = c1 * Z + onz(2 * s), c1 * Z + onz(-2 * s)
        wait(outb.at[p, far], g2sem.at[p, 0])
        send(outb.at[p, far], outb.at[p, far], p, g2sem.at[p, 4], devz(-2 * s))
        send(outb.at[p, far], outb.at[p, far], p, g2sem.at[p, 5], devz(-s))
        wait(outb.at[p, near], g2sem.at[p, 1])
        send(outb.at[p, near], outb.at[p, near], p, g2sem.at[p, 6], devz(s))

    def step7(p):
        s, c1, c3, on1, on3, onz, dev1, dev3, devz = place(p)
        for k, h in ((2, 1), (3, -1), (4, 4), (5, 3), (6, -3)):
            wait(outb.at[p, c1 * Z + onz(h * s)], g2sem.at[p, k])
        mine = outb.at[p, chunk(c1)]
        for h, o in ((0, 1), (1, -1)):
            send(mine, mine, p, g1sem.at[p, h], dev1(-o))

    def step8(p):
        s, c1, c3, on1, on3, onz, dev1, dev3, devz = place(p)
        for h, o in ((0, 1), (1, -1)):
            wait(outb.at[p, chunk(on1(o))], g1sem.at[p, h])
            one = outb.at[p, half(on1(o), h)]
            send(one, one, p, g1sem.at[p, 2 + h], dev1(-o))

    def step9(p):
        s, c1, c3, on1, on3, onz, dev1, dev3, devz = place(p)
        for h in range(2):
            wait(outb.at[p, half(on1(2), h)], g1sem.at[p, 2 + h])

    steps = [step0, step1, step2, step3, step4, step5, step6, step7, step8, step9]

    load_a(0).start()
    for t in range(GBUF - 1):
        load_g(t).start()
    for n in range(1, mats):
        load_a(n).start()

    barrier = pltpu.get_barrier_semaphore()
    _, _, _, _, _, _, devx, devy, devz = place(0)
    partners = [devx(k) for k in (1, 2, 3)] + [devy(k) for k in (1, 2, 3)] + [devz(k) for k in (-2, -1, 1, 2)]
    for dev in partners:
        pl.semaphore_signal(barrier, inc=1, device_id={"dp": dev}, device_id_type=pl.DeviceIdType.MESH)

    pl.semaphore_wait(barrier, len(partners))

    @pl.loop(0, pieces + AFTER[-1])
    def _(t):
        @pl.when(t < pieces)
        def _():
            @pl.when(t + GBUF - 1 < pieces)
            def _():
                load_g(t + GBUF - 1).start()

            compute(t)
            step0(t)

        for k in ORDER:
            p = t - AFTER[k]

            @pl.when((p >= 0) & (p < pieces))
            def _():
                steps[k](p)

    @pl.loop(0, pieces)
    def _(p):
        wait(sent_bytes(term), ssem.at[p])


def sent_bytes(term):
    return term.at[pl.ds(0, 5), pl.ds(0, 13)]


def store(panels, out_hbm, sem):
    pieces = panels.shape[0]
    per = pieces // out_hbm.shape[0]
    copies = []
    for p in range(pieces):
        for h in range(2):
            col = (p % per) * W + h * L
            src, dst = panels.at[p, pl.ds(h * (UNITS // 2), UNITS // 2)], out_hbm.at[p // per, :, :, pl.ds(col, L)]
            copies.append(pltpu.make_async_copy(src, dst, sem.at[p, h]))
    for copy in copies:
        copy.start()
    for copy in copies:
        copy.wait()


def solution(mesh):
    assert mesh.shape["dp"] == X * Y * Z

    def body(a, g):
        _, mats, tokens, d = a.shape
        ff = g.shape[3]
        pieces = mats * ff // W
        vmem = lambda *shape, dtype=bf16: pltpu.VMEM(shape, dtype)
        dma = pltpu.SemaphoreType.DMA
        panels = pl.pallas_call(
            kernel,
            name="wgrad_sums",
            out_shape=pltpu.VMEM((pieces, UNITS, U, L), bf16),
            in_specs=[pl.BlockSpec(memory_space=pl.ANY)] * 2,
            out_specs=pl.BlockSpec(memory_space=pltpu.VMEM),
            scratch_shapes=[
                vmem(mats, tokens, d),
                vmem(GBUF, tokens, W),
                vmem(pieces, UNITS, U, L),
                vmem(pieces, 6, Z // 2, U, L),
                vmem(pieces, Z, U, L, dtype=f32),
                vmem(pieces, Z, U, L),
                vmem(pieces, 7, U, L),
                vmem(pieces, 4, U, L),
                dma((mats,)),
                dma((GBUF,)),
                dma((pieces,)),
                dma((pieces, 6)),
                dma((pieces, 7)),
                dma((pieces, 3)),
                dma((pieces, 7)),
                dma((pieces, 4)),
            ],
            compiler_params=pltpu.CompilerParams(has_side_effects=True, collective_id=0, vmem_limit_bytes=50 << 20),
        )(a[0], g[0])
        out = pl.pallas_call(
            store,
            name="store_sums",
            out_shape=jax.ShapeDtypeStruct((mats, d // U, U, ff), bf16),
            in_specs=[pl.BlockSpec(memory_space=pltpu.VMEM)],
            out_specs=pl.BlockSpec(memory_space=pl.ANY),
            scratch_shapes=[dma((pieces, 2))],
            compiler_params=pltpu.CompilerParams(vmem_limit_bytes=8 << 20),
        )(panels)
        return out.reshape(mats, d, ff)

    return jax.shard_map(body, mesh=mesh, in_specs=(P(("rep", "dp")),) * 2, out_specs=P("rep"), check_vma=False)
```

```python
import jax
import jax.numpy as jnp
from jax import lax
from jax.experimental import pallas as pl
from jax.experimental.pallas import tpu as pltpu
from jax.sharding import PartitionSpec as P

X, Y, Z = 4, 4, 8
U, L = 48, 128
UNITS = 32
W = 2 * L
AFTER = (0, 3, 5, 7, 9, 12, 15, 17, 21, 26)
ORDER = (3, 2, 8, 1, 6, 5, 4, 9, 7)
GBUF = 4
MB = 384
bf16, f32 = jnp.bfloat16, jnp.float32


def kernel(a_hbm, g_hbm, outb, abuf, gbuf, term, recv1, acc, part, recv2, exch,
           asem, gsem, ssem, r1sem, r2sem, xsem, g2sem, g1sem):
    mats, tokens, d = a_hbm.shape
    per = g_hbm.shape[2] // W
    pieces = mats * per
    me = lax.axis_index("dp")
    x, y, z = me // (Y * Z), (me // Z) % Y, me % Z

    def load_a(n):
        return pltpu.make_async_copy(a_hbm.at[n], abuf.at[n], asem.at[n])

    def load_g(t):
        col = pl.multiple_of((t % per) * W, W)
        slot = t % GBUF
        return pltpu.make_async_copy(g_hbm.at[t // per, :, pl.ds(col, W)], gbuf.at[slot], gsem.at[slot])

    def compute(t):
        n, slot = t // per, t % GBUF
        load_g(t).wait()

        @pl.when(t % per == 0)
        def _():
            load_a(n).wait()

        @pl.when(t == 0)
        def _():
            for k in range(1, GBUF - 1):
                load_g(k).start()

        @pl.when(t + GBUF - 1 < pieces)
        def _():
            load_g(t + GBUF - 1).start()

        @pl.when(t % per == 1)
        def _():
            @pl.when(n + 1 < mats)
            def _():
                load_a(n + 1).start()

        for m in range(0, d, MB):
            s = lax.dot_general(abuf[n, :, m : m + MB], gbuf[slot], (((0,), (0,)), ((), ())), preferred_element_type=f32).astype(bf16)
            for h in range(2):
                u = h * (UNITS // 2) + m // U
                term[t, u : u + MB // U] = s[:, h * L : (h + 1) * L].reshape(MB // U, U, L)

    def place(p):
        odd = p % 2
        s = 1 - 2 * ((p // 2) % 2)
        c1, st1 = x + odd * (y - x), Y * Z - odd * (Y * Z - Z)
        c3, st3 = y + odd * (x - y), Z + odd * (Y * Z - Z)

        def on1(k):
            return (c1 + k + 8) % 4

        def on3(k):
            return (c3 + k + 8) % 4

        def onz(k):
            return (z + k + 8) % 8

        dev1 = lambda k: me + (on1(k) - c1) * st1
        dev3 = lambda k: me + (on3(k) - c3) * st3
        devz = lambda k: me + onz(k) - z
        return s, c1, c3, on1, on3, onz, dev1, dev3, devz

    def send(src, dst, p, sem, dev):
        pltpu.make_async_remote_copy(
            src_ref=src, dst_ref=dst, send_sem=ssem.at[p], recv_sem=sem,
            device_id={"dp": dev}, device_id_type=pl.DeviceIdType.MESH,
        ).start()

    def wait(ref, sem):
        pltpu.make_async_copy(ref, ref, sem).wait()

    def chunk(c):
        return pl.ds(c * Z, Z)

    def half(c, h):
        return pl.ds(c * Z + h * (Z // 2), Z // 2)

    def step0(p):
        s, c1, c3, on1, on3, onz, dev1, dev3, devz = place(p)
        for h, o in ((0, 1), (1, -1)):
            send(term.at[p, half(on1(2), h)], recv1.at[p, h], p, r1sem.at[p, h], dev1(-o))
        for h, o in ((0, 1), (1, -1)):
            send(term.at[p, half(on1(o), h)], recv1.at[p, 2 + h], p, r1sem.at[p, 2], dev1(o))

    def step1(p):
        s, c1, c3, on1, on3, onz, dev1, dev3, devz = place(p)
        for h, o in ((0, 1), (1, -1)):
            wait(recv1.at[p, h], r1sem.at[p, h])
            base = on1(-o) * Z + h * (Z // 2)
            for u in range(Z // 2):
                term[p, base + u] = (term[p, base + u].astype(f32) + recv1[p, h, u].astype(f32)).astype(bf16)
            send(term.at[p, half(on1(-o), h)], recv1.at[p, 4 + h], p, r1sem.at[p, 2], dev1(-o))

    def step2(p):
        s, c1, c3, on1, on3, onz, dev1, dev3, devz = place(p)
        wait(recv1.at[p, pl.ds(2, 4)], r1sem.at[p, 2])
        for u in range(Z):
            h, w = divmod(u, Z // 2)
            v = term[p, c1 * Z + u].astype(f32) + recv1[p, 2 + h, w].astype(f32) + recv1[p, 4 + h, w].astype(f32)
            acc[p, u] = v
            part[p, u] = v.astype(bf16)
        send(part.at[p, onz(4)], recv2.at[p, 0], p, r2sem.at[p, 0], devz(-2 * s))
        send(part.at[p, onz(-3 * s)], recv2.at[p, 1], p, r2sem.at[p, 0], devz(-s))
        send(part.at[p, onz(3 * s)], recv2.at[p, 2], p, r2sem.at[p, 0], devz(s))
        send(part.at[p, onz(-s)], recv2.at[p, 3], p, r2sem.at[p, 1], devz(-s))
        send(part.at[p, onz(s)], recv2.at[p, 4], p, r2sem.at[p, 1], devz(s))

    def step3(p):
        s, c1, c3, on1, on3, onz, dev1, dev3, devz = place(p)
        wait(recv2.at[p, pl.ds(0, 3)], r2sem.at[p, 0])
        far, near = onz(-2 * s), onz(2 * s)
        part[p, far] = (acc[p, far] + recv2[p, 0].astype(f32) + recv2[p, 1].astype(f32)).astype(bf16)
        part[p, near] = (acc[p, near] + recv2[p, 2].astype(f32)).astype(bf16)
        send(part.at[p, far], recv2.at[p, 5], p, r2sem.at[p, 1], devz(-2 * s))
        send(part.at[p, near], recv2.at[p, 6], p, r2sem.at[p, 1], devz(2 * s))

    def step4(p):
        s, c1, c3, on1, on3, onz, dev1, dev3, devz = place(p)
        wait(recv2.at[p, pl.ds(3, 4)], r2sem.at[p, 1])
        v = acc[p, z]
        for k in range(3, 7):
            v = v + recv2[p, k].astype(f32)
        exch[p, c3] = v.astype(bf16)
        for k in range(1, 4):
            send(exch.at[p, c3], exch.at[p, c3], p, xsem.at[p], dev3(k))

    def step5(p):
        s, c1, c3, on1, on3, onz, dev1, dev3, devz = place(p)
        wait(exch.at[p, pl.ds(0, 3)], xsem.at[p])
        v = exch[p, 0].astype(f32)
        for k in range(1, 4):
            v = v + exch[p, k].astype(f32)
        u = c1 * Z + z
        outb[p, u] = v.astype(bf16)
        for h in (-2, 2, -1, 1):
            send(outb.at[p, u], outb.at[p, u], p, g2sem.at[p, 0 if h in (-2, 2) else 1], devz(h * s))

    def step6(p):
        s, c1, c3, on1, on3, onz, dev1, dev3, devz = place(p)
        far, near = c1 * Z + onz(2 * s), c1 * Z + onz(-2 * s)
        wait(outb.at[p, pl.ds(0, 2)], g2sem.at[p, 0])
        send(outb.at[p, far], outb.at[p, far], p, g2sem.at[p, 1], devz(-2 * s))
        send(outb.at[p, far], outb.at[p, far], p, g2sem.at[p, 1], devz(-s))
        send(outb.at[p, near], outb.at[p, near], p, g2sem.at[p, 1], devz(s))

    def step7(p):
        s, c1, c3, on1, on3, onz, dev1, dev3, devz = place(p)
        wait(outb.at[p, pl.ds(0, 5)], g2sem.at[p, 1])
        for w in range(2):
            for h, o in ((0, 1), (1, -1)):
                mine = outb.at[p, half(c1, h)]
                send(mine, mine, p, g1sem.at[p, w], dev1(o * (2 * w - 1)))

    def step8(p):
        s, c1, c3, on1, on3, onz, dev1, dev3, devz = place(p)
        wait(outb.at[p, chunk(0)], g1sem.at[p, 0])
        for h, o in ((0, 1), (1, -1)):
            one = outb.at[p, half(on1(o), h)]
            send(one, one, p, g1sem.at[p, 1], dev1(-o))

    def step9(p):
        wait(outb.at[p, pl.ds(0, 2 * Z)], g1sem.at[p, 1])

    steps = [step0, step1, step2, step3, step4, step5, step6, step7, step8, step9]

    load_a(0).start()
    load_g(0).start()

    barrier = pltpu.get_barrier_semaphore()
    _, _, _, _, _, _, devx, devy, devz = place(0)
    partners = [devx(k) for k in (1, 2, 3)] + [devy(k) for k in (1, 2, 3)] + [devz(k) for k in (-2, -1, 1, 2)]
    for dev in partners:
        pl.semaphore_signal(barrier, inc=1, device_id={"dp": dev}, device_id_type=pl.DeviceIdType.MESH)

    pl.semaphore_wait(barrier, len(partners))

    @pl.loop(0, pieces + AFTER[-1])
    def _(t):
        @pl.when(t < pieces)
        def _():
            compute(t)
            step0(t)

        for k in ORDER:
            p = t - AFTER[k]

            @pl.when((p >= 0) & (p < pieces))
            def _():
                steps[k](p)

    @pl.loop(0, pieces)
    def _(p):
        wait(sent_bytes(term), ssem.at[p])


def sent_bytes(term):
    return term.at[pl.ds(0, 5), pl.ds(0, 13)]


def store(panels, out_hbm, sem):
    pieces = panels.shape[0]
    per = pieces // out_hbm.shape[0]
    copies = []
    for p in range(pieces):
        for h in range(2):
            col = (p % per) * W + h * L
            src, dst = panels.at[p, pl.ds(h * (UNITS // 2), UNITS // 2)], out_hbm.at[p // per, :, :, pl.ds(col, L)]
            copies.append(pltpu.make_async_copy(src, dst, sem.at[p, h]))
    for copy in copies:
        copy.start()
    for copy in copies:
        copy.wait()


def solution(mesh):
    assert mesh.shape["dp"] == X * Y * Z

    def body(a, g):
        _, mats, tokens, d = a.shape
        ff = g.shape[3]
        pieces = mats * ff // W
        vmem = lambda *shape, dtype=bf16: pltpu.VMEM(shape, dtype)
        dma = pltpu.SemaphoreType.DMA
        panels = pl.pallas_call(
            kernel,
            name="wgrad_sums",
            out_shape=pltpu.VMEM((pieces, UNITS, U, L), bf16),
            in_specs=[pl.BlockSpec(memory_space=pl.ANY)] * 2,
            out_specs=pl.BlockSpec(memory_space=pltpu.VMEM),
            scratch_shapes=[
                vmem(mats, tokens, d),
                vmem(GBUF, tokens, W),
                vmem(pieces, UNITS, U, L),
                vmem(pieces, 6, Z // 2, U, L),
                vmem(pieces, Z, U, L, dtype=f32),
                vmem(pieces, Z, U, L),
                vmem(pieces, 7, U, L),
                vmem(pieces, 4, U, L),
                dma((mats,)),
                dma((GBUF,)),
                dma((pieces,)),
                dma((pieces, 3)),
                dma((pieces, 2)),
                dma((pieces,)),
                dma((pieces, 2)),
                dma((pieces, 2)),
            ],
            compiler_params=pltpu.CompilerParams(has_side_effects=True, collective_id=0, vmem_limit_bytes=50 << 20),
        )(a[0], g[0])
        out = pl.pallas_call(
            store,
            name="store_sums",
            out_shape=jax.ShapeDtypeStruct((mats, d // U, U, ff), bf16),
            in_specs=[pl.BlockSpec(memory_space=pltpu.VMEM)],
            out_specs=pl.BlockSpec(memory_space=pl.ANY),
            scratch_shapes=[dma((pieces, 2))],
            compiler_params=pltpu.CompilerParams(vmem_limit_bytes=8 << 20),
        )(panels)
        return out.reshape(mats, d, ff)

    return jax.shard_map(body, mesh=mesh, in_specs=(P(("rep", "dp")),) * 2, out_specs=P("rep"), check_vma=False)
```

```python
import jax
import jax.numpy as jnp
from jax import lax
from jax.experimental import pallas as pl
from jax.experimental.pallas import tpu as pltpu
from jax.sharding import PartitionSpec as P

X, Y, Z = 4, 4, 8
U, L = 48, 128
UNITS = 32
W = 2 * L
AFTER = (0, 3, 5, 7, 9, 12, 15, 17, 20, 25)
ORDER = (3, 2, 9, 1, 6, 5, 4, 8, 7)
GBUF = 4
MB = 384
bf16, f32 = jnp.bfloat16, jnp.float32


def kernel(a_hbm, g_hbm, outb, abuf, gbuf, term, recv1, acc, part, recv2, exch,
           asem, gsem, ssem, r1sem, r2sem, xsem, g2sem, g1sem):
    mats, tokens, d = a_hbm.shape
    per = g_hbm.shape[2] // W
    pieces = mats * per
    me = lax.axis_index("dp")
    x, y, z = me // (Y * Z), (me // Z) % Y, me % Z

    def load_a(n):
        return pltpu.make_async_copy(a_hbm.at[n], abuf.at[n], asem.at[n])

    def load_g(t):
        col = pl.multiple_of((t % per) * W, W)
        slot = t % GBUF
        return pltpu.make_async_copy(g_hbm.at[t // per, :, pl.ds(col, W)], gbuf.at[slot], gsem.at[slot])

    def compute(t):
        n, slot = t // per, t % GBUF
        load_g(t).wait()

        @pl.when(t % per == 0)
        def _():
            load_a(n).wait()

        @pl.when(t == 0)
        def _():
            for k in range(1, GBUF - 1):
                load_g(k).start()

        @pl.when(t + GBUF - 1 < pieces)
        def _():
            load_g(t + GBUF - 1).start()

        @pl.when(t % per == 1)
        def _():
            @pl.when(n + 1 < mats)
            def _():
                load_a(n + 1).start()

        for m in range(0, d, MB):
            s = lax.dot_general(abuf[n, :, m : m + MB], gbuf[slot], (((0,), (0,)), ((), ())), preferred_element_type=f32).astype(bf16)
            for h in range(2):
                u = h * (UNITS // 2) + m // U
                term[t, u : u + MB // U] = s[:, h * L : (h + 1) * L].reshape(MB // U, U, L)

    def place(p):
        odd = p % 2
        s = 1 - 2 * ((p // 2) % 2)
        c1, st1 = x + odd * (y - x), Y * Z - odd * (Y * Z - Z)
        c3, st3 = y + odd * (x - y), Z + odd * (Y * Z - Z)

        def on1(k):
            return (c1 + k + 8) % 4

        def on3(k):
            return (c3 + k + 8) % 4

        def onz(k):
            return (z + k + 8) % 8

        dev1 = lambda k: me + (on1(k) - c1) * st1
        dev3 = lambda k: me + (on3(k) - c3) * st3
        devz = lambda k: me + onz(k) - z
        return s, c1, c3, on1, on3, onz, dev1, dev3, devz

    def send(src, dst, p, sem, dev):
        pltpu.make_async_remote_copy(
            src_ref=src, dst_ref=dst, send_sem=ssem.at[p], recv_sem=sem,
            device_id={"dp": dev}, device_id_type=pl.DeviceIdType.MESH,
        ).start()

    def wait(ref, sem):
        pltpu.make_async_copy(ref, ref, sem).wait()

    def chunk(c):
        return pl.ds(c * Z, Z)

    def half(c, h):
        return pl.ds(c * Z + h * (Z // 2), Z // 2)

    def step0(p):
        s, c1, c3, on1, on3, onz, dev1, dev3, devz = place(p)
        for h, o in ((0, 1), (1, -1)):
            send(term.at[p, half(on1(2), h)], recv1.at[p, h], p, r1sem.at[p, h], dev1(-o))
        for h, o in ((0, 1), (1, -1)):
            send(term.at[p, half(on1(o), h)], recv1.at[p, 2 + h], p, r1sem.at[p, 2], dev1(o))

    def step1(p):
        s, c1, c3, on1, on3, onz, dev1, dev3, devz = place(p)
        for h, o in ((0, 1), (1, -1)):
            wait(recv1.at[p, h], r1sem.at[p, h])
            base = on1(-o) * Z + h * (Z // 2)
            for u in range(Z // 2):
                term[p, base + u] = (term[p, base + u].astype(f32) + recv1[p, h, u].astype(f32)).astype(bf16)
            send(term.at[p, half(on1(-o), h)], recv1.at[p, 4 + h], p, r1sem.at[p, 2], dev1(-o))

    def step2(p):
        s, c1, c3, on1, on3, onz, dev1, dev3, devz = place(p)
        wait(recv1.at[p, pl.ds(2, 4)], r1sem.at[p, 2])
        for u in range(Z):
            h, w = divmod(u, Z // 2)
            v = term[p, c1 * Z + u].astype(f32) + recv1[p, 2 + h, w].astype(f32) + recv1[p, 4 + h, w].astype(f32)
            acc[p, u] = v
            part[p, u] = v.astype(bf16)
        send(part.at[p, onz(4)], recv2.at[p, 0], p, r2sem.at[p, 0], devz(-2 * s))
        send(part.at[p, onz(-3 * s)], recv2.at[p, 1], p, r2sem.at[p, 0], devz(-s))
        send(part.at[p, onz(3 * s)], recv2.at[p, 2], p, r2sem.at[p, 0], devz(s))
        send(part.at[p, onz(-s)], recv2.at[p, 3], p, r2sem.at[p, 1], devz(-s))
        send(part.at[p, onz(s)], recv2.at[p, 4], p, r2sem.at[p, 1], devz(s))

    def step3(p):
        s, c1, c3, on1, on3, onz, dev1, dev3, devz = place(p)
        wait(recv2.at[p, pl.ds(0, 3)], r2sem.at[p, 0])
        far, near = onz(-2 * s), onz(2 * s)
        part[p, far] = (acc[p, far] + recv2[p, 0].astype(f32) + recv2[p, 1].astype(f32)).astype(bf16)
        part[p, near] = (acc[p, near] + recv2[p, 2].astype(f32)).astype(bf16)
        send(part.at[p, far], recv2.at[p, 5], p, r2sem.at[p, 1], devz(-2 * s))
        send(part.at[p, near], recv2.at[p, 6], p, r2sem.at[p, 1], devz(2 * s))

    def step4(p):
        s, c1, c3, on1, on3, onz, dev1, dev3, devz = place(p)
        wait(recv2.at[p, pl.ds(3, 4)], r2sem.at[p, 1])
        v = acc[p, z]
        for k in range(3, 7):
            v = v + recv2[p, k].astype(f32)
        exch[p, c3] = v.astype(bf16)
        for k in (2, 1, 3):
            send(exch.at[p, c3], exch.at[p, c3], p, xsem.at[p], dev3(k))

    def step5(p):
        s, c1, c3, on1, on3, onz, dev1, dev3, devz = place(p)
        wait(exch.at[p, pl.ds(0, 3)], xsem.at[p])
        v = exch[p, 0].astype(f32)
        for k in range(1, 4):
            v = v + exch[p, k].astype(f32)
        u = c1 * Z + z
        outb[p, u] = v.astype(bf16)
        for h in (-2, 2, -1, 1):
            send(outb.at[p, u], outb.at[p, u], p, g2sem.at[p, 0 if h in (-2, 2) else 1], devz(h * s))

    def step6(p):
        s, c1, c3, on1, on3, onz, dev1, dev3, devz = place(p)
        far, near = c1 * Z + onz(2 * s), c1 * Z + onz(-2 * s)
        wait(outb.at[p, pl.ds(0, 2)], g2sem.at[p, 0])
        send(outb.at[p, far], outb.at[p, far], p, g2sem.at[p, 1], devz(-2 * s))
        send(outb.at[p, far], outb.at[p, far], p, g2sem.at[p, 1], devz(-s))
        send(outb.at[p, near], outb.at[p, near], p, g2sem.at[p, 1], devz(s))

    def step7(p):
        s, c1, c3, on1, on3, onz, dev1, dev3, devz = place(p)
        wait(outb.at[p, pl.ds(0, 5)], g2sem.at[p, 1])
        for w in range(2):
            for h, o in ((0, 1), (1, -1)):
                mine = outb.at[p, half(c1, h)]
                send(mine, mine, p, g1sem.at[p, w], dev1(o * (2 * w - 1)))

    def step8(p):
        s, c1, c3, on1, on3, onz, dev1, dev3, devz = place(p)
        wait(outb.at[p, chunk(0)], g1sem.at[p, 0])
        for h, o in ((0, 1), (1, -1)):
            one = outb.at[p, half(on1(o), h)]
            send(one, one, p, g1sem.at[p, 1], dev1(-o))

    def step9(p):
        wait(outb.at[p, pl.ds(0, 2 * Z)], g1sem.at[p, 1])

    steps = [step0, step1, step2, step3, step4, step5, step6, step7, step8, step9]

    load_a(0).start()
    load_g(0).start()

    barrier = pltpu.get_barrier_semaphore()
    _, _, _, _, _, _, devx, devy, devz = place(0)
    partners = [devx(k) for k in (1, 2, 3)] + [devy(k) for k in (1, 2, 3)] + [devz(k) for k in (-2, -1, 1, 2)]
    for dev in partners:
        pl.semaphore_signal(barrier, inc=1, device_id={"dp": dev}, device_id_type=pl.DeviceIdType.MESH)

    pl.semaphore_wait(barrier, len(partners))

    @pl.loop(0, pieces + AFTER[-1])
    def _(t):
        @pl.when(t < pieces)
        def _():
            compute(t)
            step0(t)

        for k in ORDER:
            p = t - AFTER[k]

            @pl.when((p >= 0) & (p < pieces))
            def _():
                steps[k](p)

    @pl.loop(0, pieces)
    def _(p):
        wait(sent_bytes(term), ssem.at[p])


def sent_bytes(term):
    return term.at[pl.ds(0, 5), pl.ds(0, 13)]


def store(panels, out_hbm, sem):
    pieces = panels.shape[0]
    per = pieces // out_hbm.shape[0]
    copies = []
    for p in range(pieces):
        for h in range(2):
            col = (p % per) * W + h * L
            src, dst = panels.at[p, pl.ds(h * (UNITS // 2), UNITS // 2)], out_hbm.at[p // per, :, :, pl.ds(col, L)]
            copies.append(pltpu.make_async_copy(src, dst, sem.at[p, h]))
    for copy in copies:
        copy.start()
    for copy in copies:
        copy.wait()


def solution(mesh):
    assert mesh.shape["dp"] == X * Y * Z

    def body(a, g):
        _, mats, tokens, d = a.shape
        ff = g.shape[3]
        pieces = mats * ff // W
        vmem = lambda *shape, dtype=bf16: pltpu.VMEM(shape, dtype)
        dma = pltpu.SemaphoreType.DMA
        panels = pl.pallas_call(
            kernel,
            name="wgrad_sums",
            out_shape=pltpu.VMEM((pieces, UNITS, U, L), bf16),
            in_specs=[pl.BlockSpec(memory_space=pl.ANY)] * 2,
            out_specs=pl.BlockSpec(memory_space=pltpu.VMEM),
            scratch_shapes=[
                vmem(mats, tokens, d),
                vmem(GBUF, tokens, W),
                vmem(pieces, UNITS, U, L),
                vmem(pieces, 6, Z // 2, U, L),
                vmem(pieces, Z, U, L, dtype=f32),
                vmem(pieces, Z, U, L),
                vmem(pieces, 7, U, L),
                vmem(pieces, 4, U, L),
                dma((mats,)),
                dma((GBUF,)),
                dma((pieces,)),
                dma((pieces, 3)),
                dma((pieces, 2)),
                dma((pieces,)),
                dma((pieces, 2)),
                dma((pieces, 2)),
            ],
            compiler_params=pltpu.CompilerParams(has_side_effects=True, collective_id=0, vmem_limit_bytes=50 << 20),
        )(a[0], g[0])
        out = pl.pallas_call(
            store,
            name="store_sums",
            out_shape=jax.ShapeDtypeStruct((mats, d // U, U, ff), bf16),
            in_specs=[pl.BlockSpec(memory_space=pltpu.VMEM)],
            out_specs=pl.BlockSpec(memory_space=pl.ANY),
            scratch_shapes=[dma((pieces, 2))],
            compiler_params=pltpu.CompilerParams(vmem_limit_bytes=8 << 20),
        )(panels)
        return out.reshape(mats, d, ff)

    return jax.shard_map(body, mesh=mesh, in_specs=(P(("rep", "dp")),) * 2, out_specs=P("rep"), check_vma=False)
```
